32 devices in a mesh: row: 16 (over z, x, core), col: 2 (over y).
Axes of the slice: x: 2, y: 2, z: 4, core: 2. Of those that a mesh axis runs over, the one named last changes fastest.
Arguments:
- sequence_embedding: float32 [128, 64, 256], P('row', 'col'), may hold values from -6 to 6
- standardize_scale: float32 [256], replicated, may hold values from 0.25 to 1.75
- standardize_offset: float32 [256], replicated, may hold values from -0.5 to 0.5
- first_operand_matrix: float32 [256, 32], replicated, may hold values from -0.375 to 0.375
- first_operand_intercept: float32 [32], replicated, may hold values from -0.5 to 0.5
- second_operand_matrix: float32 [256, 32], replicated, may hold values from -0.375 to 0.375
- second_operand_intercept: float32 [32], replicated, may hold values from -0.5 to 0.5
- result_matrix: float32 [1024, 128], replicated, may hold values from -2 to 2
- result_intercept: float32 [128], replicated, may hold values from -0.5 to 0.5
- edge_incoming_sensitivity: float32 [64, 64, 128], P('row', 'col'), may hold values from -6 to 6
Outputs:
- pair_output_update: float32 [64, 64, 128], P('row', 'col')
- alignment_gradient: float32 [128, 64, 256], P('row', 'col')
- projection_gradient: float32 [1024, 128], P(('row', 'col'))
The draws below stay inside these ranges and needn't reach their ends.
All inputs are finite; a program needn't handle non-finite values.
Results may differ from the reference program's by a relative error of at most 0.0001.
Values sent between devices are 32-bit elements; how exact they have to be, the bound alone decides.
A program may use at most 64 MiB of HBM per device.

```python
import math
import jax
import jax.numpy as jnp
from jax import lax

SEQUENCE_FEATS = 256
HIDDEN_WIDTH = 32
EDGE_FEATURES = 128
SEQUENCE_COUNT = 128
SEQUENCE_SPAN = 64


def block_scale(key, extent, pieces, smallest, high):
    def one(axis_at, blocks):
        heights = jax.random.uniform(jax.random.fold_in(jax.random.fold_in(key, 6), axis_at), (blocks,), jnp.float32, smallest / len(pieces), high / len(pieces))
        return jnp.repeat(jnp.exp(heights), extent[axis_at] // blocks).reshape((-1,) + (1,) * (len(extent) - axis_at - 1))

    loudness = one(*pieces[0])
    for cut in pieces[1:]:
        loudness = loudness * one(*cut)
    return loudness


def bell_draw(stream_key, shape, width, bound, shards=(), held_as=jnp.bfloat16):
    drawn = jax.random.normal(stream_key, shape, jnp.float32) * width
    if len(shards) > 0:
        drawn = block_scale(stream_key, shape, shards, -0.22, 0.18) * drawn
    return jnp.clip(drawn, min=-bound, max=bound).astype(held_as)


def setup_inputs(seed: int = 0) -> dict:
    splits = jax.random.split(jax.random.key(seed), 11)
    sequence_embedding = bell_draw(splits[0], (SEQUENCE_COUNT, SEQUENCE_SPAN, SEQUENCE_FEATS), 1.0, 6.0, ((0, 16), (1, 2)), jnp.float32)
    standardize_scale = jnp.clip(1.0 + 0.15 * jax.random.normal(splits[1], (SEQUENCE_FEATS,), jnp.float32), 0.25, 1.75)
    standardize_offset = jnp.clip(jax.random.uniform(splits[2], (SEQUENCE_FEATS,), jnp.float32, -0.5, 0.5), -0.5, 0.5)
    first_operand_matrix = bell_draw(splits[3], (SEQUENCE_FEATS, HIDDEN_WIDTH), SEQUENCE_FEATS ** -0.5, 0.375, (), jnp.float32)
    first_operand_intercept = jnp.clip(jax.random.uniform(splits[4], (HIDDEN_WIDTH,), jnp.float32, -0.5, 0.5), -0.5, 0.5)
    second_operand_matrix = bell_draw(splits[5], (SEQUENCE_FEATS, HIDDEN_WIDTH), SEQUENCE_FEATS ** -0.5, 0.375, (), jnp.float32)
    second_operand_intercept = jnp.clip(jax.random.uniform(splits[6], (HIDDEN_WIDTH,), jnp.float32, -0.5, 0.5), -0.5, 0.5)
    result_matrix = bell_draw(splits[7], (HIDDEN_WIDTH * HIDDEN_WIDTH, EDGE_FEATURES), (HIDDEN_WIDTH * HIDDEN_WIDTH // SEQUENCE_COUNT) ** -0.5, 2.0, (), jnp.float32)
    result_intercept = jnp.clip(jax.random.uniform(splits[8], (EDGE_FEATURES,), jnp.float32, -0.5, 0.5), -0.5, 0.5)
    edge_incoming_sensitivity = bell_draw(splits[9], (SEQUENCE_SPAN, SEQUENCE_SPAN, EDGE_FEATURES), 1.0, 6.0, ((0, 16), (1, 2)), jnp.float32)
    return dict(sequence_embedding=sequence_embedding, standardize_scale=standardize_scale, standardize_offset=standardize_offset, first_operand_matrix=first_operand_matrix, first_operand_intercept=first_operand_intercept, second_operand_matrix=second_operand_matrix, second_operand_intercept=second_operand_intercept, result_matrix=result_matrix, result_intercept=result_intercept, edge_incoming_sensitivity=edge_incoming_sensitivity)


precise = lax.Precision.HIGHEST

def linear_transform(sequence_embedding, standardize_scale, standardize_offset, first_operand_matrix, first_operand_intercept, second_operand_matrix, second_operand_intercept):
    average_feature = lax.optimization_barrier(jnp.mean(sequence_embedding, axis=-1, keepdims=True))
    demeaned_features = sequence_embedding - average_feature
    variance = lax.optimization_barrier(jnp.mean(demeaned_features * demeaned_features, axis=-1, keepdims=True))
    normed = demeaned_features * lax.rsqrt(variance + 1e-05) * standardize_scale + standardize_offset
    first_operand_entries = jnp.einsum('src,cd->srd', normed, first_operand_matrix, precision=precise) + first_operand_intercept
    second_operand_entries = jnp.einsum('src,cd->srd', normed, second_operand_matrix, precision=precise) + second_operand_intercept
    return (first_operand_entries, second_operand_entries)

def tile_work(left_all, right_all, result_matrix, result_intercept, edge_incoming_sensitivity):
    rows_all, tile_i, chans = left_all.shape
    tile_j = right_all.shape[1]
    pair_ch = result_matrix.shape[1]
    block_rows = math.gcd(tile_i, 8)
    num_blocks = tile_i // block_rows
    left_blocks = left_all.reshape(rows_all, num_blocks, block_rows, chans).transpose(1, 0, 2, 3)
    cot_blocks = edge_incoming_sensitivity.reshape(num_blocks, block_rows, tile_j, pair_ch)

    def tile_step(carry, inputs):
        summed_weight, right_sum = carry
        left_blk, cot_blk = inputs
        products = jnp.einsum('sic,sje->ijce', left_blk, right_all, precision=precise)
        products = products.reshape(block_rows, tile_j, chans * chans)
        pair_blk = jnp.einsum('ijk,kh->ijh', products, result_matrix, precision=precise) / rows_all + result_intercept
        grad_outer = jnp.einsum('ijh,kh->ijk', cot_blk, result_matrix, precision=precise) / rows_all
        grad_outer = grad_outer.reshape(block_rows, tile_j, chans, chans)
        summed_weight = summed_weight + jnp.einsum('ijk,ijh->kh', products, cot_blk, precision=precise)
        left_factor_gradient = jnp.einsum('ijce,sje->sic', grad_outer, right_all, precision=precise)
        right_sum = right_sum + jnp.einsum('sic,ijce->sje', left_blk, grad_outer, precision=precise)
        return ((summed_weight, right_sum), (pair_blk, left_factor_gradient))
    initial = (jnp.zeros((chans * chans, pair_ch), jnp.float32), jnp.zeros(right_all.shape, jnp.float32))
    (summed_weight, right_sum), (pair_blocks, left_grads) = lax.scan(tile_step, initial, (left_blocks, cot_blocks))
    pair_tile = pair_blocks.reshape(tile_i, tile_j, pair_ch)
    left_factor_gradient = left_grads.transpose(1, 0, 2, 3).reshape(rows_all, tile_i, chans)
    return (pair_tile, left_factor_gradient, summed_weight, right_sum)

def reference(sequence_embedding, standardize_scale, standardize_offset, first_operand_matrix, first_operand_intercept, second_operand_matrix, second_operand_intercept, result_matrix, result_intercept, edge_incoming_sensitivity):

    def device_portion(values):
        return linear_transform(values, standardize_scale, standardize_offset, first_operand_matrix, first_operand_intercept, second_operand_matrix, second_operand_intercept)
    (first_operand_entries, second_operand_entries), reverse_derivative = jax.vjp(device_portion, sequence_embedding)
    pair_output_update, left_factor_gradient, summed_weight, right_factor_gradient = tile_work(first_operand_entries, second_operand_entries, result_matrix, result_intercept, edge_incoming_sensitivity)
    alignment_gradient = reverse_derivative((left_factor_gradient, right_factor_gradient))[0]
    return (pair_output_update, alignment_gradient, summed_weight / SEQUENCE_SPAN)
```

```python
import functools

import jax
import jax.numpy as jnp
from jax import lax
from jax.experimental import pallas as pl
from jax.experimental.pallas import tpu as pltpu
from jax.sharding import PartitionSpec as P

MESH = pl.DeviceIdType.MESH
LANES = 128

NN = (((1,), (0,)), ((), ()))
NT = (((1,), (1,)), ((), ()))
TN = (((0,), (0,)), ((), ()))


def split(a):
    hi = a.astype(jnp.bfloat16)
    return hi, (a - hi.astype(jnp.float32)).astype(jnp.bfloat16)


def mul(a, b, dims):
    (ah, al), (bh, bl) = a, b
    one = functools.partial(lax.dot_general, dimension_numbers=dims, preferred_element_type=jnp.float32)
    return one(ah, bh) + (one(ah, bl) + one(al, bh))


def block_transpose(parts, width):
    parts = list(parts)
    count = len(parts)
    block = lax.broadcasted_iota(jnp.int32, parts[0].shape, 1) // width
    half = count // 2
    while half >= 1:
        low = (block & half) == 0
        for a in range(count):
            if a & half:
                continue
            va, vb = parts[a], parts[a + half]
            parts[a] = jnp.where(low, va, pltpu.roll(vb, half * width, 1))
            parts[a + half] = jnp.where(low, pltpu.roll(va, LANES - half * width, 1), vb)
        half //= 2
    return parts


def kernel(
    n_row, n_col, s_loc, tile_i, tile_j, chans,
    x_ref, scale_ref, offset_ref, w1_ref, b1_ref, w2_ref, b2_ref, wr_ref, br_ref, cot_ref,
    pair_ref, ag_ref, proj_ref,
    xs, xhat, rstd, mixl, mixr, wt, rsend, lsend, r_all, l_all, wp, mt, gt, outer, pp, psend, precv,
    rgrad, lgrad, rrecv, lrecv, send_sems, recv_sems, bar_sems,
):
    row, col = lax.axis_index("row"), lax.axis_index("col")
    n_dev = n_row * n_col
    me = row * n_col + col
    rows_all = n_row * s_loc
    feats = x_ref.shape[1]
    q = LANES // chans
    groups = tile_j // q
    per_col = tile_j // tile_i
    owner = row // per_col
    place = row % per_col
    rp = proj_ref.shape[0]

    barrier = pltpu.get_barrier_semaphore()

    @pl.loop(1, n_dev)
    def _(d):
        t = lax.rem(me + d, n_dev)
        pl.semaphore_signal(barrier, inc=1, device_id=(t // n_col, lax.rem(t, n_col)), device_id_type=MESH)

    lane_block = lax.broadcasted_iota(jnp.int32, (feats, LANES), 1) // chans
    w1t = jnp.concatenate([w1_ref[...]] * q, axis=1)
    w2t = jnp.concatenate([w2_ref[...]] * q, axis=1)
    accl = jnp.concatenate([b1_ref[...]] * q, axis=1)
    accr = jnp.concatenate([b2_ref[...]] * q, axis=1)
    acc = jnp.concatenate([accl, accr], axis=1)
    for h in range(feats // LANES):
        xs[h] = x_ref[:, h * LANES : (h + 1) * LANES]
    for k in range(q):
        wk = jnp.concatenate(
            [jnp.where(lane_block == k, w1t, 0.0), jnp.where(lane_block == k, w2t, 0.0)], axis=1
        )
        wt[k] = wk
        halves = [
            xs[h, pl.ds(k, s_loc * groups, stride=q), :] for h in range(feats // LANES)
        ]
        xk = jnp.concatenate(halves, axis=1)
        dk = xk - jnp.mean(xk, axis=1, keepdims=True)
        rk = lax.rsqrt(jnp.mean(dk * dk, axis=1, keepdims=True) + 1e-05)
        hat = dk * rk
        xhat[k] = hat
        rstd[k] = rk
        acc = acc + mul(split(hat * scale_ref[...] + offset_ref[...]), split(wk), NN)
    mixl[...] = acc[:, :LANES]
    mixr[...] = acc[:, LANES:]
    for g in range(groups):
        rsend[:, g * LANES : (g + 1) * LANES] = mixr[pl.ds(g, s_loc, stride=groups), :]
        b, off = (g * q) // tile_i, (g * q) % tile_i * chans
        lsend[b, :, off : off + LANES] = mixl[pl.ds(g, s_loc, stride=groups), :]

    pl.semaphore_wait(barrier, n_dev - 1)

    @pl.loop(1, n_row)
    def _(d):
        t = lax.rem(row + d, n_row)
        pltpu.make_async_remote_copy(
            src_ref=rsend, dst_ref=r_all.at[row], send_sem=send_sems.at[0], recv_sem=recv_sems.at[0],
            device_id=(t, col), device_id_type=MESH,
        ).start()

    def send_left(b, c):
        pltpu.make_async_remote_copy(
            src_ref=lsend.at[b], dst_ref=l_all.at[row], send_sem=send_sems.at[1], recv_sem=recv_sems.at[1],
            device_id=(col * per_col + b, c), device_id_type=MESH,
        ).start()

    mine = owner == col

    @pl.loop(0, per_col)
    def _(b):
        @pl.loop(0, n_col)
        def _(c):
            other = jnp.logical_or(c != col, col * per_col + b != row)

            @pl.when(other)
            def _():
                send_left(b, c)

    r_all[row] = rsend[...]

    @pl.when(mine)
    def _():
        l_all[row] = lsend[place]

    for e in range(chans):
        wp[pl.ds(e * chans, chans), :] = wr_ref[pl.ds(e, chans, stride=chans), :]
    cots = split(cot_ref[...])
    wps = split(wp[...])
    outer[...] = mul(cots, wps, NT) * (1.0 / rows_all)
    for ig in range(tile_i // q):
        for eg in range(chans // q):
            parts = [
                outer[(ig * q + k) * tile_j : (ig * q + k + 1) * tile_j, eg * LANES : (eg + 1) * LANES]
                for k in range(q)
            ]
            for k, part in enumerate(block_transpose(parts, chans)):
                gt[ig, pl.ds(eg * q + k, tile_j, stride=chans), :] = part
    gts = split(jnp.concatenate([gt[ig] for ig in range(tile_i // q)], axis=1))

    def wait(ref, sem):
        pltpu.make_async_copy(ref, ref, sem).wait()

    wait(r_all.at[pl.ds(0, n_row - 1)], recv_sems.at[0])

    @pl.when(mine)
    def _():
        wait(l_all.at[pl.ds(0, n_row - 1)], recv_sems.at[1])

    @pl.when(jnp.logical_not(mine))
    def _():
        wait(l_all, recv_sems.at[1])

    right = split(r_all[...].reshape(rows_all, tile_j * chans))
    left = split(l_all[...].reshape(rows_all, tile_i * chans))
    product = mul(right, left, TN)
    for ig in range(tile_i // q):
        mt[ig] = product[:, ig * LANES : (ig + 1) * LANES]
    for ig in range(tile_i // q):
        for eg in range(chans // q):
            parts = [
                mt[ig, pl.ds(eg * q + k, tile_j, stride=chans), :] for k in range(q)
            ]
            for k, part in enumerate(block_transpose(parts, chans)):
                outer[(ig * q + k) * tile_j : (ig * q + k + 1) * tile_j, eg * LANES : (eg + 1) * LANES] = part
    outers = split(outer[...])
    pp[...] = mul(outers, cots, TN)
    per = chans // rp
    for c in range(chans):
        rows = pp[pl.ds(c, chans, stride=chans), :]
        for t in range(per):
            psend[c * per + t] = rows[t * rp : (t + 1) * rp]

    @pl.loop(1, n_dev)
    def _(d):
        t = lax.rem(me + d, n_dev)
        pltpu.make_async_remote_copy(
            src_ref=psend.at[t], dst_ref=precv.at[me], send_sem=send_sems.at[2], recv_sem=recv_sems.at[2],
            device_id=(t // n_col, lax.rem(t, n_col)), device_id_type=MESH,
        ).start()

    rgrad[...] = mul(left, gts, NT).reshape(n_row, s_loc, tile_j * chans)

    @pl.loop(1, n_row)
    def _(d):
        t = lax.rem(row + d, n_row)
        pltpu.make_async_remote_copy(
            src_ref=rgrad.at[t], dst_ref=rrecv.at[row], send_sem=send_sems.at[3], recv_sem=recv_sems.at[3],
            device_id=(t, col), device_id_type=MESH,
        ).start()

    lgrad[...] = mul(right, gts, NN).reshape(n_row, s_loc, tile_i * chans)

    @pl.loop(0, n_row)
    def _(t):
        @pl.when(jnp.logical_or(t != row, owner != col))
        def _():
            pltpu.make_async_remote_copy(
                src_ref=lgrad.at[t], dst_ref=lrecv.at[col * per_col + place],
                send_sem=send_sems.at[4], recv_sem=recv_sems.at[4],
                device_id=(t, owner), device_id_type=MESH,
            ).start()

    pair_ref[...] = mul(outers, wps, NN) * (1.0 / rows_all) + br_ref[...]

    precv[me] = psend[me]
    rrecv[row] = rgrad[row]

    @pl.when(mine)
    def _():
        lrecv[col * per_col + place] = lgrad[row]

    wait(rrecv.at[pl.ds(0, n_row - 1)], recv_sems.at[3])

    @pl.when(mine)
    def _():
        wait(lrecv.at[pl.ds(0, n_row - 1)], recv_sems.at[4])

    @pl.when(jnp.logical_not(mine))
    def _():
        wait(lrecv, recv_sems.at[4])

    rsum = jnp.sum(rrecv[...], axis=0)
    lsum = lrecv[pl.ds(0, per_col)]
    for c in range(1, n_col):
        lsum = lsum + lrecv[pl.ds(c * per_col, per_col)]
    for g in range(groups):
        b, off = (g * q) // tile_i, (g * q) % tile_i * chans
        mixr[pl.ds(g, s_loc, stride=groups), :] = rsum[:, g * LANES : (g + 1) * LANES]
        mixl[pl.ds(g, s_loc, stride=groups), :] = lsum[b, :, off : off + LANES]
    grads = split(jnp.concatenate([mixl[...], mixr[...]], axis=1))
    for k in range(q):
        dk = mul(grads, split(wt[k]), NT) * scale_ref[...]
        hat = xhat[k]
        back = rstd[k] * (
            dk - jnp.mean(dk, axis=1, keepdims=True) - hat * jnp.mean(dk * hat, axis=1, keepdims=True)
        )
        for h in range(feats // LANES):
            xs[h, pl.ds(k, s_loc * groups, stride=q), :] = back[:, h * LANES : (h + 1) * LANES]
    for h in range(feats // LANES):
        ag_ref[:, h * LANES : (h + 1) * LANES] = xs[h]

    wait(precv.at[pl.ds(0, n_dev - 1)], recv_sems.at[2])
    proj_ref[...] = jnp.sum(precv[...], axis=0) * (1.0 / (tile_j * n_col))

    wait(r_all.at[pl.ds(0, n_row - 1)], send_sems.at[0])

    @pl.when(mine)
    def _():
        wait(l_all.at[pl.ds(0, per_col * n_col - 1)], send_sems.at[1])
        wait(lrecv.at[pl.ds(0, n_row - 1)], send_sems.at[4])

    @pl.when(jnp.logical_not(mine))
    def _():
        wait(l_all, send_sems.at[1])
        wait(lrecv, send_sems.at[4])

    wait(precv.at[pl.ds(0, n_dev - 1)], send_sems.at[2])
    wait(rrecv.at[pl.ds(0, n_row - 1)], send_sems.at[3])


def solution(mesh):
    n_row, n_col = mesh.shape["row"], mesh.shape["col"]
    n_dev = n_row * n_col

    def local(x, scale, offset, w1, b1, w2, b2, wr, br, cot):
        s_loc, tile_j, feats = x.shape
        tile_i, _, pair_ch = cot.shape
        chans = w1.shape[1]
        rows_all = n_row * s_loc
        q = LANES // chans
        groups = tile_j // q
        per_col = tile_j // tile_i
        rp = chans * chans // n_dev
        f32 = jnp.float32
        vm = lambda *shape: pltpu.VMEM(shape, f32)
        wide, thin = tile_j * chans, tile_i * chans
        pair, grad, proj = pl.pallas_call(
            functools.partial(kernel, n_row, n_col, s_loc, tile_i, tile_j, chans),
            out_shape=(
                jax.ShapeDtypeStruct((tile_i * tile_j, pair_ch), f32),
                jax.ShapeDtypeStruct((s_loc * tile_j, feats), f32),
                jax.ShapeDtypeStruct((rp, pair_ch), f32),
            ),
            in_specs=[pl.BlockSpec(memory_space=pltpu.VMEM)] * 10,
            out_specs=(pl.BlockSpec(memory_space=pltpu.VMEM),) * 3,
            scratch_shapes=[
                vm(feats // LANES, s_loc * tile_j, LANES),
                vm(q, s_loc * groups, feats),
                vm(q, s_loc * groups, 1),
                vm(s_loc * groups, LANES),
                vm(s_loc * groups, LANES),
                vm(q, feats, 2 * LANES),
                vm(s_loc, wide),
                vm(per_col, s_loc, thin),
                vm(n_row, s_loc, wide),
                vm(n_row, s_loc, thin),
                vm(chans * chans, pair_ch),
                vm(tile_i // q, wide, LANES),
                vm(tile_i // q, wide, LANES),
                vm(tile_i * tile_j, chans * chans),
                vm(chans * chans, pair_ch),
                vm(n_dev, rp, pair_ch),
                vm(n_dev, rp, pair_ch),
                vm(n_row, s_loc, wide),
                vm(n_row, s_loc, thin),
                vm(n_row, s_loc, wide),
                vm(n_col * per_col, s_loc, thin),
                pltpu.SemaphoreType.DMA((5,)),
                pltpu.SemaphoreType.DMA((5,)),
                pltpu.SemaphoreType.DMA((1,)),
            ],
            compiler_params=pltpu.CompilerParams(
                collective_id=0, has_side_effects=True, vmem_limit_bytes=60 * 1024 * 1024
            ),
        )(
            x.reshape(s_loc * tile_j, feats), scale.reshape(1, -1), offset.reshape(1, -1),
            w1, b1.reshape(1, -1), w2, b2.reshape(1, -1), wr, br.reshape(1, -1),
            cot.reshape(tile_i * tile_j, pair_ch),
        )
        return (
            pair.reshape(tile_i, tile_j, pair_ch),
            grad.reshape(s_loc, tile_j, feats),
            proj,
        )

    return jax.shard_map(
        local,
        mesh=mesh,
        in_specs=(
            P("row", "col", None), P(), P(), P(), P(), P(), P(), P(), P(), P("row", "col", None),
        ),
        out_specs=(P("row", "col", None), P("row", "col", None), P(("row", "col"), None)),
        check_vma=False,
    )
```

```python
import functools

import jax
import jax.numpy as jnp
from jax import lax
from jax.experimental import pallas as pl
from jax.experimental.pallas import tpu as pltpu
from jax.sharding import PartitionSpec as P

MESH = pl.DeviceIdType.MESH
LANES = 128

NN = (((1,), (0,)), ((), ()))
NT = (((1,), (1,)), ((), ()))
TN = (((0,), (0,)), ((), ()))


def split(a):
    hi = a.astype(jnp.bfloat16)
    return hi, (a - hi.astype(jnp.float32)).astype(jnp.bfloat16)


def mul(a, b, dims):
    (ah, al), (bh, bl) = a, b
    one = functools.partial(lax.dot_general, dimension_numbers=dims, preferred_element_type=jnp.float32)
    return one(ah, bh) + (one(ah, bl) + one(al, bh))


def block_transpose(parts, width):
    parts = list(parts)
    count = len(parts)
    block = lax.broadcasted_iota(jnp.int32, parts[0].shape, 1) // width
    half = count // 2
    while half >= 1:
        low = (block & half) == 0
        for a in range(count):
            if a & half:
                continue
            va, vb = parts[a], parts[a + half]
            parts[a] = jnp.where(low, va, pltpu.roll(vb, half * width, 1))
            parts[a + half] = jnp.where(low, pltpu.roll(va, LANES - half * width, 1), vb)
        half //= 2
    return parts


def kernel(
    n_row, n_col, s_loc, tile_i, tile_j, chans,
    x_ref, scale_ref, offset_ref, w1_ref, b1_ref, w2_ref, b2_ref, wr_ref, br_ref, cot_ref,
    pair_ref, ag_ref, proj_ref,
    xs, xhat, rstd, mixl, mixr, wt, rsend, lsend, r_all, l_all, wp, mt, gt, outer, pp, psend, pmid, pout, precv,
    rgrad, rmid, rout, lgrad, rrecv, lrecv, send_sems, recv_sems,
):
    row, col = lax.axis_index("row"), lax.axis_index("col")
    n_dev = n_row * n_col
    me = row * n_col + col
    rows_all = n_row * s_loc
    feats = x_ref.shape[1]
    q = LANES // chans
    groups = tile_j // q
    per_col = tile_j // tile_i
    owner = row // per_col
    place = row % per_col
    rp = proj_ref.shape[0]
    core, chip, n_chip = row % 2, row // 2, n_row // 2
    slot = core * n_chip + chip
    partner = (row + 1 - 2 * core, col)
    half = n_chip * n_col
    spot = chip * n_col + col

    barrier = pltpu.get_barrier_semaphore()

    @pl.loop(1, n_dev)
    def _(d):
        t = lax.rem(me + d, n_dev)
        pl.semaphore_signal(barrier, inc=1, device_id=(t // n_col, lax.rem(t, n_col)), device_id_type=MESH)

    accl = jnp.concatenate([b1_ref[...]] * q, axis=1)
    accr = jnp.concatenate([b2_ref[...]] * q, axis=1)
    acc = jnp.concatenate([accl, accr], axis=1)
    for h in range(feats // LANES):
        xs[h] = x_ref[:, h * LANES : (h + 1) * LANES]
    for k in range(q):
        blank = jnp.zeros((chans, feats), jnp.float32)
        pieces = [blank] * (2 * q)
        pieces[k], pieces[q + k] = w1_ref[...], w2_ref[...]
        wk = jnp.concatenate(pieces, axis=0)
        wt[k] = wk
        halves = [
            xs[h, pl.ds(k, s_loc * groups, stride=q), :] for h in range(feats // LANES)
        ]
        xk = jnp.concatenate(halves, axis=1)
        dk = xk - jnp.mean(xk, axis=1, keepdims=True)
        rk = lax.rsqrt(jnp.mean(dk * dk, axis=1, keepdims=True) + 1e-05)
        hat = dk * rk
        xhat[k] = hat
        rstd[k] = rk
        acc = acc + mul(split(hat * scale_ref[...] + offset_ref[...]), split(wk), NT)
    mixl[...] = acc[:, :LANES]
    mixr[...] = acc[:, LANES:]
    for g in range(groups):
        rsend[:, g * LANES : (g + 1) * LANES] = mixr[pl.ds(g, s_loc, stride=groups), :]
        b, off = (g * q) // tile_i, (g * q) % tile_i * chans
        lsend[b, :, off : off + LANES] = mixl[pl.ds(g, s_loc, stride=groups), :]

    pl.semaphore_wait(barrier, n_dev - 1)

    def send_left(b, c):
        pltpu.make_async_remote_copy(
            src_ref=lsend.at[b], dst_ref=l_all.at[slot], send_sem=send_sems.at[1], recv_sem=recv_sems.at[1],
            device_id=(col * per_col + b, c), device_id_type=MESH,
        ).start()

    mine = owner == col

    @pl.loop(0, per_col)
    def _(b):
        @pl.loop(0, n_col)
        def _(c):
            other = jnp.logical_or(c != col, col * per_col + b != row)

            @pl.when(other)
            def _():
                send_left(b, c)

    @pl.loop(1, n_chip)
    def _(d):
        t = lax.rem(chip + d, n_chip)
        pltpu.make_async_remote_copy(
            src_ref=rsend, dst_ref=r_all.at[slot], send_sem=send_sems.at[0], recv_sem=recv_sems.at[0],
            device_id=(t * 2 + core, col), device_id_type=MESH,
        ).start()

    r_all[slot] = rsend[...]

    @pl.when(mine)
    def _():
        l_all[slot] = lsend[place]

    for e in range(chans):
        wp[pl.ds(e * chans, chans), :] = wr_ref[pl.ds(e, chans, stride=chans), :]
    cots = split(cot_ref[...])
    wps = split(wp[...])
    outer[...] = mul(cots, wps, NT) * (1.0 / rows_all)
    for ig in range(tile_i // q):
        for eg in range(chans // q):
            parts = [
                outer[(ig * q + k) * tile_j : (ig * q + k + 1) * tile_j, eg * LANES : (eg + 1) * LANES]
                for k in range(q)
            ]
            for k, part in enumerate(block_transpose(parts, chans)):
                gt[ig, pl.ds(eg * q + k, tile_j, stride=chans), :] = part
    gts = split(jnp.concatenate([gt[ig] for ig in range(tile_i // q)], axis=1))

    def wait(ref, sem):
        pltpu.make_async_copy(ref, ref, sem).wait()

    @pl.when(mine)
    def _():
        wait(l_all.at[pl.ds(0, n_row - 1)], recv_sems.at[1])

    @pl.when(jnp.logical_not(mine))
    def _():
        wait(l_all, recv_sems.at[1])

    left = split(l_all[...].reshape(rows_all, tile_i * chans))
    rgrad[...] = mul(left, gts, NT).reshape(n_row, s_loc, tile_j * chans)

    def to_partner(src, dst, at):
        pltpu.make_async_remote_copy(
            src_ref=src, dst_ref=dst, send_sem=send_sems.at[at], recv_sem=recv_sems.at[at],
            device_id=partner, device_id_type=MESH,
        ).start()

    to_partner(rgrad.at[pl.ds((1 - core) * n_chip, n_chip)], rmid, 5)
    wait(rmid, recv_sems.at[5])
    rout[...] = rgrad[pl.ds(core * n_chip, n_chip)] + rmid[...]

    @pl.loop(1, n_chip)
    def _(d):
        t = lax.rem(chip + d, n_chip)
        pltpu.make_async_remote_copy(
            src_ref=rout.at[t], dst_ref=rrecv.at[chip], send_sem=send_sems.at[3], recv_sem=recv_sems.at[3],
            device_id=(t * 2 + core, col), device_id_type=MESH,
        ).start()

    rrecv[chip] = rout[chip]

    wait(r_all.at[pl.ds(0, n_chip - 1)], recv_sems.at[0])
    shared = r_all.at[pl.ds(core * n_chip, n_chip)]
    to_partner(shared, shared, 6)
    wait(r_all.at[pl.ds(0, n_chip)], recv_sems.at[6])
    right = split(r_all[...].reshape(rows_all, tile_j * chans))
    product = mul(right, left, TN)
    for ig in range(tile_i // q):
        mt[ig] = product[:, ig * LANES : (ig + 1) * LANES]
    for ig in range(tile_i // q):
        for eg in range(chans // q):
            parts = [
                mt[ig, pl.ds(eg * q + k, tile_j, stride=chans), :] for k in range(q)
            ]
            for k, part in enumerate(block_transpose(parts, chans)):
                outer[(ig * q + k) * tile_j : (ig * q + k + 1) * tile_j, eg * LANES : (eg + 1) * LANES] = part
    outers = split(outer[...])
    pp[...] = mul(outers, cots, TN)
    per = chans // rp
    for c in range(chans):
        rows = pp[pl.ds(c, chans, stride=chans), :]
        for t in range(per):
            p = c * per + t
            place_of = p // n_col % 2 * half + p // n_col // 2 * n_col + p % n_col
            psend[place_of] = rows[t * rp : (t + 1) * rp]

    to_partner(psend.at[pl.ds((1 - core) * half, half)], pmid, 7)
    lgrad[...] = mul(right, gts, NN).reshape(n_row, s_loc, tile_i * chans)

    @pl.loop(0, n_row)
    def _(t):
        @pl.when(jnp.logical_or(t != row, owner != col))
        def _():
            pltpu.make_async_remote_copy(
                src_ref=lgrad.at[(t % 2) * n_chip + t // 2], dst_ref=lrecv.at[col * per_col + place],
                send_sem=send_sems.at[4], recv_sem=recv_sems.at[4],
                device_id=(t, owner), device_id_type=MESH,
            ).start()

    wait(pmid, recv_sems.at[7])
    pout[...] = psend[pl.ds(core * half, half)] + pmid[...]

    @pl.loop(1, half)
    def _(d):
        t = lax.rem(spot + d, half)
        pltpu.make_async_remote_copy(
            src_ref=pout.at[t], dst_ref=precv.at[spot], send_sem=send_sems.at[2], recv_sem=recv_sems.at[2],
            device_id=(t // n_col * 2 + core, lax.rem(t, n_col)), device_id_type=MESH,
        ).start()

    pair_ref[...] = mul(outers, wps, NN) * (1.0 / rows_all) + br_ref[...]

    precv[spot] = pout[spot]

    @pl.when(mine)
    def _():
        lrecv[col * per_col + place] = lgrad[slot]

    wait(rrecv.at[pl.ds(0, n_chip - 1)], recv_sems.at[3])

    @pl.when(mine)
    def _():
        wait(lrecv.at[pl.ds(0, n_row - 1)], recv_sems.at[4])

    @pl.when(jnp.logical_not(mine))
    def _():
        wait(lrecv, recv_sems.at[4])

    rsum = jnp.sum(rrecv[...], axis=0)
    lsum = lrecv[pl.ds(0, per_col)]
    for c in range(1, n_col):
        lsum = lsum + lrecv[pl.ds(c * per_col, per_col)]
    for g in range(groups):
        b, off = (g * q) // tile_i, (g * q) % tile_i * chans
        mixr[pl.ds(g, s_loc, stride=groups), :] = rsum[:, g * LANES : (g + 1) * LANES]
        mixl[pl.ds(g, s_loc, stride=groups), :] = lsum[b, :, off : off + LANES]
    grads = split(jnp.concatenate([mixl[...], mixr[...]], axis=1))
    for k in range(q):
        dk = mul(grads, split(wt[k]), NN) * scale_ref[...]
        hat = xhat[k]
        back = rstd[k] * (
            dk - jnp.mean(dk, axis=1, keepdims=True) - hat * jnp.mean(dk * hat, axis=1, keepdims=True)
        )
        for h in range(feats // LANES):
            xs[h, pl.ds(k, s_loc * groups, stride=q), :] = back[:, h * LANES : (h + 1) * LANES]
    for h in range(feats // LANES):
        ag_ref[:, h * LANES : (h + 1) * LANES] = xs[h]

    wait(precv.at[pl.ds(0, half - 1)], recv_sems.at[2])
    proj_ref[...] = jnp.sum(precv[...], axis=0) * (1.0 / (tile_j * n_col))

    wait(r_all.at[pl.ds(0, n_chip - 1)], send_sems.at[0])
    wait(rmid, send_sems.at[5])
    wait(shared, send_sems.at[6])
    wait(pmid, send_sems.at[7])

    @pl.when(mine)
    def _():
        wait(l_all.at[pl.ds(0, per_col * n_col - 1)], send_sems.at[1])
        wait(lrecv.at[pl.ds(0, n_row - 1)], send_sems.at[4])

    @pl.when(jnp.logical_not(mine))
    def _():
        wait(l_all, send_sems.at[1])
        wait(lrecv, send_sems.at[4])

    wait(precv.at[pl.ds(0, half - 1)], send_sems.at[2])
    wait(rrecv.at[pl.ds(0, n_chip - 1)], send_sems.at[3])


def solution(mesh):
    n_row, n_col = mesh.shape["row"], mesh.shape["col"]
    n_dev = n_row * n_col

    def local(x, scale, offset, w1, b1, w2, b2, wr, br, cot):
        s_loc, tile_j, feats = x.shape
        tile_i, _, pair_ch = cot.shape
        chans = w1.shape[1]
        rows_all = n_row * s_loc
        q = LANES // chans
        groups = tile_j // q
        per_col = tile_j // tile_i
        rp = chans * chans // n_dev
        f32 = jnp.float32
        vm = lambda *shape: pltpu.VMEM(shape, f32)
        wide, thin = tile_j * chans, tile_i * chans
        pair, grad, proj = pl.pallas_call(
            functools.partial(kernel, n_row, n_col, s_loc, tile_i, tile_j, chans),
            out_shape=(
                jax.ShapeDtypeStruct((tile_i * tile_j, pair_ch), f32),
                jax.ShapeDtypeStruct((s_loc * tile_j, feats), f32),
                jax.ShapeDtypeStruct((rp, pair_ch), f32),
            ),
            in_specs=[pl.BlockSpec(memory_space=pltpu.VMEM)] * 10,
            out_specs=(pl.BlockSpec(memory_space=pltpu.VMEM),) * 3,
            scratch_shapes=[
                vm(feats // LANES, s_loc * tile_j, LANES),
                vm(q, s_loc * groups, feats),
                vm(q, s_loc * groups, 1),
                vm(s_loc * groups, LANES),
                vm(s_loc * groups, LANES),
                vm(q, 2 * LANES, feats),
                vm(s_loc, wide),
                vm(per_col, s_loc, thin),
                vm(n_row, s_loc, wide),
                vm(n_row, s_loc, thin),
                vm(chans * chans, pair_ch),
                vm(tile_i // q, wide, LANES),
                vm(tile_i // q, wide, LANES),
                vm(tile_i * tile_j, chans * chans),
                vm(chans * chans, pair_ch),
                vm(n_dev, rp, pair_ch),
                vm(n_dev // 2, rp, pair_ch),
                vm(n_dev // 2, rp, pair_ch),
                vm(n_dev // 2, rp, pair_ch),
                vm(n_row, s_loc, wide),
                vm(n_row // 2, s_loc, wide),
                vm(n_row // 2, s_loc, wide),
                vm(n_row, s_loc, thin),
                vm(n_row // 2, s_loc, wide),
                vm(n_col * per_col, s_loc, thin),
                pltpu.SemaphoreType.DMA((8,)),
                pltpu.SemaphoreType.DMA((8,)),
            ],
            compiler_params=pltpu.CompilerParams(
                collective_id=0, has_side_effects=True, vmem_limit_bytes=60 * 1024 * 1024
            ),
        )(
            x.reshape(s_loc * tile_j, feats), scale.reshape(1, -1), offset.reshape(1, -1),
            w1.T, b1.reshape(1, -1), w2.T, b2.reshape(1, -1), wr, br.reshape(1, -1),
            cot.reshape(tile_i * tile_j, pair_ch),
        )
        return (
            pair.reshape(tile_i, tile_j, pair_ch),
            grad.reshape(s_loc, tile_j, feats),
            proj,
        )

    return jax.shard_map(
        local,
        mesh=mesh,
        in_specs=(
            P("row", "col", None), P(), P(), P(), P(), P(), P(), P(), P(), P("row", "col", None),
        ),
        out_specs=(P("row", "col", None), P("row", "col", None), P(("row", "col"), None)),
        check_vma=False,
    )
```

```python
import functools

import jax
import jax.numpy as jnp
from jax import lax
from jax.experimental import pallas as pl
from jax.experimental.pallas import tpu as pltpu
from jax.sharding import PartitionSpec as P

MESH = pl.DeviceIdType.MESH
LANES = 128

NN = (((1,), (0,)), ((), ()))
NT = (((1,), (1,)), ((), ()))
TN = (((0,), (0,)), ((), ()))


def split(a):
    hi = a.astype(jnp.bfloat16)
    return hi, (a - hi.astype(jnp.float32)).astype(jnp.bfloat16)


def mul(a, b, dims):
    (ah, al), (bh, bl) = a, b
    one = functools.partial(lax.dot_general, dimension_numbers=dims, preferred_element_type=jnp.float32)
    return one(ah, bh) + (one(ah, bl) + one(al, bh))


def block_transpose(parts, width):
    parts = list(parts)
    count = len(parts)
    block = lax.broadcasted_iota(jnp.int32, parts[0].shape, 1) // width
    half = count // 2
    while half >= 1:
        low = (block & half) == 0
        for a in range(count):
            if a & half:
                continue
            va, vb = parts[a], parts[a + half]
            parts[a] = jnp.where(low, va, pltpu.roll(vb, half * width, 1))
            parts[a + half] = jnp.where(low, pltpu.roll(va, LANES - half * width, 1), vb)
        half //= 2
    return parts


def kernel(
    n_row, n_col, s_loc, tile_i, tile_j, chans,
    x_ref, scale_ref, offset_ref, w1_ref, b1_ref, w2_ref, b2_ref, wr_ref, cot_ref,
    pair_ref, ag_ref, proj_ref,
    xs, xhat, rstd, mixl, mixr, wt, rsend, lsend, r_all, l_all, wp, mt, gt, outer, pp, psend, pmid, pout, precv,
    rgrad, rmid, rout, lgrad, rrecv, lrecv, send_sems, recv_sems,
):
    row, col = lax.axis_index("row"), lax.axis_index("col")
    n_dev = n_row * n_col
    me = row * n_col + col
    rows_all = n_row * s_loc
    feats = x_ref.shape[1]
    q = LANES // chans
    groups = tile_j // q
    per_col = tile_j // tile_i
    owner = row // per_col
    place = row % per_col
    rp = proj_ref.shape[0]
    core, chip, n_chip = row % 2, row // 2, n_row // 2
    slot = core * n_chip + chip
    partner = (row + 1 - 2 * core, col)
    half = n_chip * n_col
    spot = chip * n_col + col

    barrier = pltpu.get_barrier_semaphore()

    @pl.loop(1, n_dev)
    def _(d):
        t = lax.rem(me + d, n_dev)
        pl.semaphore_signal(barrier, inc=1, device_id=(t // n_col, lax.rem(t, n_col)), device_id_type=MESH)

    accl = jnp.concatenate([b1_ref[...]] * q, axis=1)
    accr = jnp.concatenate([b2_ref[...]] * q, axis=1)
    acc = jnp.concatenate([accl, accr], axis=1)
    for h in range(feats // LANES):
        xs[h] = x_ref[:, h * LANES : (h + 1) * LANES]
    for k in range(q):
        blank = jnp.zeros((chans, feats), jnp.float32)
        pieces = [blank] * (2 * q)
        pieces[k], pieces[q + k] = w1_ref[...], w2_ref[...]
        wk = jnp.concatenate(pieces, axis=0)
        wt[k] = wk
        halves = [
            xs[h, pl.ds(k, s_loc * groups, stride=q), :] for h in range(feats // LANES)
        ]
        xk = jnp.concatenate(halves, axis=1)
        dk = xk - jnp.mean(xk, axis=1, keepdims=True)
        rk = lax.rsqrt(jnp.mean(dk * dk, axis=1, keepdims=True) + 1e-05)
        hat = dk * rk
        xhat[k] = hat
        rstd[k] = rk
        acc = acc + mul(split(hat * scale_ref[...] + offset_ref[...]), split(wk), NT)
    mixl[...] = acc[:, :LANES]
    mixr[...] = acc[:, LANES:]
    for g in range(groups):
        rsend[:, g * LANES : (g + 1) * LANES] = mixr[pl.ds(g, s_loc, stride=groups), :]
        b, off = (g * q) // tile_i, (g * q) % tile_i * chans
        lsend[b, :, off : off + LANES] = mixl[pl.ds(g, s_loc, stride=groups), :]

    pl.semaphore_wait(barrier, n_dev - 1)

    def send_left(b, c):
        pltpu.make_async_remote_copy(
            src_ref=lsend.at[b], dst_ref=l_all.at[slot], send_sem=send_sems.at[1], recv_sem=recv_sems.at[1],
            device_id=(col * per_col + b, c), device_id_type=MESH,
        ).start()

    mine = owner == col

    @pl.loop(0, per_col)
    def _(b):
        @pl.loop(0, n_col)
        def _(c):
            other = jnp.logical_or(c != col, col * per_col + b != row)

            @pl.when(other)
            def _():
                send_left(b, c)

    @pl.loop(1, n_chip)
    def _(d):
        t = lax.rem(chip + d, n_chip)
        pltpu.make_async_remote_copy(
            src_ref=rsend, dst_ref=r_all.at[slot], send_sem=send_sems.at[0], recv_sem=recv_sems.at[0],
            device_id=(t * 2 + core, col), device_id_type=MESH,
        ).start()

    r_all[slot] = rsend[...]

    @pl.when(mine)
    def _():
        l_all[slot] = lsend[place]

    for e in range(chans):
        wp[pl.ds(e * chans, chans), :] = wr_ref[pl.ds(e, chans, stride=chans), :]
    cots = split(cot_ref[...])
    wps = split(wp[...])
    outer[...] = mul(cots, wps, NT) * (1.0 / rows_all)
    for ig in range(tile_i // q):
        for eg in range(chans // q):
            parts = [
                outer[(ig * q + k) * tile_j : (ig * q + k + 1) * tile_j, eg * LANES : (eg + 1) * LANES]
                for k in range(q)
            ]
            for k, part in enumerate(block_transpose(parts, chans)):
                gt[ig, pl.ds(eg * q + k, tile_j, stride=chans), :] = part
    gts = split(jnp.concatenate([gt[ig] for ig in range(tile_i // q)], axis=1))

    def wait(ref, sem):
        pltpu.make_async_copy(ref, ref, sem).wait()

    @pl.when(mine)
    def _():
        wait(l_all.at[pl.ds(0, n_row - 1)], recv_sems.at[1])

    @pl.when(jnp.logical_not(mine))
    def _():
        wait(l_all, recv_sems.at[1])

    left = split(l_all[...].reshape(rows_all, tile_i * chans))
    rgrad[...] = mul(left, gts, NT).reshape(n_row, s_loc, tile_j * chans)

    def to_partner(src, dst, at):
        pltpu.make_async_remote_copy(
            src_ref=src, dst_ref=dst, send_sem=send_sems.at[at], recv_sem=recv_sems.at[at],
            device_id=partner, device_id_type=MESH,
        ).start()

    to_partner(rgrad.at[pl.ds((1 - core) * n_chip, n_chip)], rmid, 5)
    wait(rmid, recv_sems.at[5])
    rout[...] = rgrad[pl.ds(core * n_chip, n_chip)] + rmid[...]

    @pl.loop(1, n_chip)
    def _(d):
        t = lax.rem(chip + d, n_chip)
        pltpu.make_async_remote_copy(
            src_ref=rout.at[t], dst_ref=rrecv.at[chip], send_sem=send_sems.at[3], recv_sem=recv_sems.at[3],
            device_id=(t * 2 + core, col), device_id_type=MESH,
        ).start()

    rrecv[chip] = rout[chip]

    wait(r_all.at[pl.ds(0, n_chip - 1)], recv_sems.at[0])
    shared = r_all.at[pl.ds(core * n_chip, n_chip)]
    to_partner(shared, shared, 6)
    wait(r_all.at[pl.ds(0, n_chip)], recv_sems.at[6])
    right = split(r_all[...].reshape(rows_all, tile_j * chans))
    product = mul(right, left, TN)
    for ig in range(tile_i // q):
        mt[ig] = product[:, ig * LANES : (ig + 1) * LANES]
    for ig in range(tile_i // q):
        for eg in range(chans // q):
            parts = [
                mt[ig, pl.ds(eg * q + k, tile_j, stride=chans), :] for k in range(q)
            ]
            for k, part in enumerate(block_transpose(parts, chans)):
                outer[(ig * q + k) * tile_j : (ig * q + k + 1) * tile_j, eg * LANES : (eg + 1) * LANES] = part
    outers = split(outer[...])
    pp[...] = mul(outers, cots, TN)
    per = chans // rp
    for c in range(chans):
        rows = pp[pl.ds(c, chans, stride=chans), :]
        for t in range(per):
            p = c * per + t
            place_of = p // n_col % 2 * half + p // n_col // 2 * n_col + p % n_col
            psend[place_of] = rows[t * rp : (t + 1) * rp]

    to_partner(psend.at[pl.ds((1 - core) * half, half)], pmid, 7)
    lgrad[...] = mul(right, gts, NN).reshape(n_row, s_loc, tile_i * chans)

    @pl.loop(0, n_row)
    def _(t):
        @pl.when(jnp.logical_or(t != row, owner != col))
        def _():
            pltpu.make_async_remote_copy(
                src_ref=lgrad.at[(t % 2) * n_chip + t // 2], dst_ref=lrecv.at[col * per_col + place],
                send_sem=send_sems.at[4], recv_sem=recv_sems.at[4],
                device_id=(t, owner), device_id_type=MESH,
            ).start()

    wait(pmid, recv_sems.at[7])
    pout[...] = psend[pl.ds(core * half, half)] + pmid[...]

    @pl.loop(1, half)
    def _(d):
        t = lax.rem(spot + d, half)
        pltpu.make_async_remote_copy(
            src_ref=pout.at[t], dst_ref=precv.at[spot], send_sem=send_sems.at[2], recv_sem=recv_sems.at[2],
            device_id=(t // n_col * 2 + core, lax.rem(t, n_col)), device_id_type=MESH,
        ).start()

    pair_ref[...] = mul(outers, wps, NN)

    precv[spot] = pout[spot]

    @pl.when(mine)
    def _():
        lrecv[col * per_col + place] = lgrad[slot]

    wait(rrecv.at[pl.ds(0, n_chip - 1)], recv_sems.at[3])

    @pl.when(mine)
    def _():
        wait(lrecv.at[pl.ds(0, n_row - 1)], recv_sems.at[4])

    @pl.when(jnp.logical_not(mine))
    def _():
        wait(lrecv, recv_sems.at[4])

    rsum = jnp.sum(rrecv[...], axis=0)
    lsum = lrecv[pl.ds(0, per_col)]
    for c in range(1, n_col):
        lsum = lsum + lrecv[pl.ds(c * per_col, per_col)]
    for g in range(groups):
        b, off = (g * q) // tile_i, (g * q) % tile_i * chans
        mixr[pl.ds(g, s_loc, stride=groups), :] = rsum[:, g * LANES : (g + 1) * LANES]
        mixl[pl.ds(g, s_loc, stride=groups), :] = lsum[b, :, off : off + LANES]
    grads = split(jnp.concatenate([mixl[...], mixr[...]], axis=1))
    for k in range(q):
        dk = mul(grads, split(wt[k]), NN) * scale_ref[...]
        hat = xhat[k]
        back = rstd[k] * (
            dk - jnp.mean(dk, axis=1, keepdims=True) - hat * jnp.mean(dk * hat, axis=1, keepdims=True)
        )
        for h in range(feats // LANES):
            xs[h, pl.ds(k, s_loc * groups, stride=q), :] = back[:, h * LANES : (h + 1) * LANES]
    for h in range(feats // LANES):
        ag_ref[:, h * LANES : (h + 1) * LANES] = xs[h]

    wait(precv.at[pl.ds(0, half - 1)], recv_sems.at[2])
    proj_ref[...] = jnp.sum(precv[...], axis=0)

    wait(r_all.at[pl.ds(0, n_chip - 1)], send_sems.at[0])
    wait(rmid, send_sems.at[5])
    wait(shared, send_sems.at[6])
    wait(pmid, send_sems.at[7])

    @pl.when(mine)
    def _():
        wait(l_all.at[pl.ds(0, per_col * n_col - 1)], send_sems.at[1])
        wait(lrecv.at[pl.ds(0, n_row - 1)], send_sems.at[4])

    @pl.when(jnp.logical_not(mine))
    def _():
        wait(l_all, send_sems.at[1])
        wait(lrecv, send_sems.at[4])

    wait(precv.at[pl.ds(0, half - 1)], send_sems.at[2])
    wait(rrecv.at[pl.ds(0, n_chip - 1)], send_sems.at[3])


def finish(rows_all, span, pair_ref, grad_ref, proj_ref, br_ref, pair_out, grad_out, proj_out):
    pair_out[...] = pair_ref[...] * (1.0 / rows_all) + br_ref[...]
    grad_out[...] = grad_ref[...]
    proj_out[...] = proj_ref[...] * (1.0 / span)


def solution(mesh):
    n_row, n_col = mesh.shape["row"], mesh.shape["col"]
    n_dev = n_row * n_col

    def local(x, scale, offset, w1, b1, w2, b2, wr, br, cot):
        s_loc, tile_j, feats = x.shape
        tile_i, _, pair_ch = cot.shape
        chans = w1.shape[1]
        rows_all = n_row * s_loc
        q = LANES // chans
        groups = tile_j // q
        per_col = tile_j // tile_i
        rp = chans * chans // n_dev
        f32 = jnp.float32
        vm = lambda *shape: pltpu.VMEM(shape, f32)
        wide, thin = tile_j * chans, tile_i * chans
        pair, grad, proj = pl.pallas_call(
            functools.partial(kernel, n_row, n_col, s_loc, tile_i, tile_j, chans),
            out_shape=(
                jax.ShapeDtypeStruct((tile_i * tile_j, pair_ch), f32),
                jax.ShapeDtypeStruct((s_loc * tile_j, feats), f32),
                jax.ShapeDtypeStruct((rp, pair_ch), f32),
            ),
            in_specs=[pl.BlockSpec(memory_space=pltpu.VMEM)] * 9,
            out_specs=(pl.BlockSpec(memory_space=pltpu.VMEM),) * 3,
            scratch_shapes=[
                vm(feats // LANES, s_loc * tile_j, LANES),
                vm(q, s_loc * groups, feats),
                vm(q, s_loc * groups, 1),
                vm(s_loc * groups, LANES),
                vm(s_loc * groups, LANES),
                vm(q, 2 * LANES, feats),
                vm(s_loc, wide),
                vm(per_col, s_loc, thin),
                vm(n_row, s_loc, wide),
                vm(n_row, s_loc, thin),
                vm(chans * chans, pair_ch),
                vm(tile_i // q, wide, LANES),
                vm(tile_i // q, wide, LANES),
                vm(tile_i * tile_j, chans * chans),
                vm(chans * chans, pair_ch),
                vm(n_dev, rp, pair_ch),
                vm(n_dev // 2, rp, pair_ch),
                vm(n_dev // 2, rp, pair_ch),
                vm(n_dev // 2, rp, pair_ch),
                vm(n_row, s_loc, wide),
                vm(n_row // 2, s_loc, wide),
                vm(n_row // 2, s_loc, wide),
                vm(n_row, s_loc, thin),
                vm(n_row // 2, s_loc, wide),
                vm(n_col * per_col, s_loc, thin),
                pltpu.SemaphoreType.DMA((8,)),
                pltpu.SemaphoreType.DMA((8,)),
            ],
            compiler_params=pltpu.CompilerParams(
                collective_id=0, has_side_effects=True, vmem_limit_bytes=60 * 1024 * 1024
            ),
        )(
            x.reshape(s_loc * tile_j, feats), scale.reshape(1, -1), offset.reshape(1, -1),
            w1.T, b1.reshape(1, -1), w2.T, b2.reshape(1, -1), wr,
            cot.reshape(tile_i * tile_j, pair_ch),
        )
        pair, grad, proj = pl.pallas_call(
            functools.partial(finish, rows_all, tile_j * n_col),
            out_shape=tuple(jax.ShapeDtypeStruct(a.shape, f32) for a in (pair, grad, proj)),
            in_specs=[pl.BlockSpec(memory_space=pltpu.VMEM)] * 4,
            out_specs=(pl.BlockSpec(memory_space=pltpu.VMEM),) * 3,
        )(pair, grad, proj, br.reshape(1, -1))
        return (
            pair.reshape(tile_i, tile_j, pair_ch),
            grad.reshape(s_loc, tile_j, feats),
            proj,
        )

    return jax.shard_map(
        local,
        mesh=mesh,
        in_specs=(
            P("row", "col", None), P(), P(), P(), P(), P(), P(), P(), P(), P("row", "col", None),
        ),
        out_specs=(P("row", "col", None), P("row", "col", None), P(("row", "col"), None)),
        check_vma=False,
    )
```
